32 devices in a mesh: gx: 8 (over y, x, core), gy: 4 (over z).
Axes of the slice: x: 2, y: 2, z: 4, core: 2. Of those that a mesh axis runs over, the one named last changes fastest.
Arguments:
- obstacles: int32 [1024, 1024], P('gx', 'gy'), may hold values 0 or 1
- load: float32 [1024, 1024], P('gx', 'gy'), may hold values from 0.25 to 4
- exit_rows: int32 [4, 256], replicated, may hold values from 0 to 1023
- exit_cols: int32 [4, 256], replicated, may hold values from 0 to 1023
Outputs:
- potential: float32 [4, 1024, 1024], P(None, 'gx', 'gy')
The draws below stay inside these ranges and needn't reach their ends.
All inputs are finite; a program needn't handle non-finite values. No bound on the sum of `obstacles` on one device may be relied on, other than what follows from the above.
Results may differ from the reference program's by a relative error of at most 0.0001.
Values sent between devices are 32-bit elements; how exact they have to be, the bound alone decides.
A program may use at most 64 MiB of HBM per device.

```python
import jax
import jax.numpy as jnp

GOALS = 4
COARSEN = 4
SMOOTH = 4
CSWEEPS = 4
CYCLES = 2
NX = 1024
NY = 1024
EXITS = 256


def draw_load(key, part):
    rough_part = jax.random.uniform(key, (NX, NY), jnp.float32, 0.25, 2.0)
    return rough_part


def touch_ends(values, own_key, smallest, largest):
    index_at = [jax.random.randint(jax.random.fold_in(own_key, axis), (), 0, length) for axis, length in enumerate(values.shape)]
    main_axis = values.shape.index(max(values.shape))
    beside = index_at[:main_axis] + [(index_at[main_axis] + 1) % values.shape[main_axis]] + index_at[main_axis + 1:]
    return values.at[tuple(index_at)].set(smallest).at[tuple(beside)].set(largest)


def setup_inputs(seed: int = 0) -> dict:
    key_of = jax.random.split(jax.random.key(seed), 5)
    return {
        "obstacles": touch_ends((jax.random.randint(key_of[0], (NX, NY), 0, 5) < 1).astype(jnp.int32), jax.random.fold_in(key_of[0], 1), 0, 1),
        "load": draw_load(jax.random.fold_in(key_of[4], 71), 0),
        "exit_rows": touch_ends(jax.random.randint(key_of[2], (GOALS, EXITS), 0, NX), jax.random.fold_in(key_of[2], 1), 0, NX - 1).astype(jnp.int32),
        "exit_cols": touch_ends(jax.random.randint(key_of[3], (GOALS, EXITS), 0, NY), jax.random.fold_in(key_of[3], 1), 0, NY - 1).astype(jnp.int32),
    }


SCREENING = 1e-4
EXIT_SINK = 4.0
COARSE_SHIFT = 0.01
DAMPING = 0.8
UPPER_BOUND = 12.5
LOWER_BOUND = 1.0


def cross_sum(field):
    padded = jnp.pad(field, ((0, 0), (1, 1), (1, 1)))
    return padded[:, 2:, 1:-1] + padded[:, :-2, 1:-1] + padded[:, 1:-1, 2:] + padded[:, 1:-1, :-2]


def chebyshev(start, residual, operate):
    center = 0.5 * (UPPER_BOUND + LOWER_BOUND)
    half_span = 0.5 * (UPPER_BOUND - LOWER_BOUND)
    sigma_ratio = center / half_span
    ratio_old = 1.0 / sigma_ratio
    update = residual / center
    result = start + update
    for sweep in range(SMOOTH - 1):
        residual = residual - operate(update)
        ratio_new = 1.0 / (2.0 * sigma_ratio - ratio_old)
        update = (ratio_new * ratio_old) * update + (2.0 * ratio_new / half_span) * residual
        result = result + update
        ratio_old = ratio_new
    return result


def restrict(residual):
    goals, height, width = residual.shape
    blocks = residual.reshape(goals, height // COARSEN, COARSEN, width // COARSEN, COARSEN)
    return blocks.mean(axis=(2, 4))


def coarse_solve(coarse_rhs):
    center_weight = 4.0 + COARSE_SHIFT
    estimate = DAMPING * coarse_rhs / center_weight
    for sweep in range(CSWEEPS - 1):
        estimate = estimate + DAMPING * (coarse_rhs - (center_weight * estimate - cross_sum(estimate))) / center_weight
    return estimate


def prolong(estimate, open_cells):
    expanded = jnp.repeat(jnp.repeat(estimate, COARSEN, axis=1), COARSEN, axis=2)
    return open_cells * expanded


def reference(obstacles, load, exit_rows, exit_cols):
    open_cells = (1 - obstacles).astype(jnp.float32)
    neighbours = cross_sum(open_cells[None])[0]
    goals = exit_rows.shape[0]
    flat_index = (exit_rows * NY + exit_cols).astype(jnp.int32)
    goal_index = jnp.broadcast_to(jnp.arange(goals, dtype=jnp.int32)[:, None], flat_index.shape)
    marks = jnp.zeros((goals, NX * NY), jnp.float32).at[goal_index, flat_index].add(1.0)
    exits = jnp.minimum(marks, 1.0).reshape(goals, NX, NY)
    diagonal = SCREENING + 4.0 * (1.0 - open_cells) + open_cells * neighbours + EXIT_SINK * open_cells * exits

    def operate(field):
        return diagonal * field - open_cells * cross_sum(open_cells * field)

    source = jnp.broadcast_to(open_cells * load, (goals, NX, NY))
    potential = chebyshev(jnp.zeros_like(source), source, operate)
    estimate = coarse_solve(restrict(source))
    for cycle in range(1, CYCLES):
        correction = prolong(estimate, open_cells)
        residual = source - operate(potential)
        shifted = residual - operate(correction)
        estimate_next = coarse_solve(restrict(residual))
        potential = chebyshev(potential + correction, shifted, operate)
        estimate = estimate_next
    return potential + prolong(estimate, open_cells)
```

```python
import functools

import jax
import jax.numpy as jnp
from jax import lax
from jax.experimental import pallas as pl
from jax.experimental.pallas import tpu as pltpu
from jax.sharding import PartitionSpec as P

COARSEN = 4
SMOOTH = 4
CSWEEPS = 4

SCREENING = 0.0001
EXIT_SINK = 4.0
COARSE_SHIFT = 0.01
DAMPING = 0.8
UPPER_BOUND = 12.5
LOWER_BOUND = 1.0

CENTER = 0.5 * (UPPER_BOUND + LOWER_BOUND)
LANES = 128
SUB = 8
HALO = COARSEN * CSWEEPS
COARSE_HALO = HALO // COARSEN

DIRECTIONS = ((-1, 0), (1, 0), (0, -1), (0, 1), (-1, -1), (-1, 1), (1, -1), (1, 1))


def smoother_coefficients():
    def add(p, q):
        size = max(len(p), len(q))
        p, q = p + [0.0] * (size - len(p)), q + [0.0] * (size - len(q))
        return [a + b for a, b in zip(p, q)]

    def scale(k, p):
        return [k * a for a in p]

    half_span = 0.5 * (UPPER_BOUND - LOWER_BOUND)
    sigma_ratio = CENTER / half_span
    ratio_old = 1.0 / sigma_ratio
    residual = [1.0]
    update = scale(1.0 / CENTER, residual)
    result = update
    for sweep in range(SMOOTH - 1):
        applied = scale(CENTER, add(update, scale(-1.0, [0.0] + update)))
        residual = add(residual, scale(-1.0, applied))
        ratio_new = 1.0 / (2.0 * sigma_ratio - ratio_old)
        update = add(
            scale(ratio_new * ratio_old, update), scale(2.0 * ratio_new / half_span, residual)
        )
        result = add(result, update)
        ratio_old = ratio_new
    return result


def lane_iota(rows):
    return lax.broadcasted_iota(jnp.int32, (rows, LANES), 1)


def exchange_kernel(
    peers, obst_ref, load_ref, out_ref, top, bot, lef, rig, from_rows, from_cols, from_corners,
    send_sem, recv_sem,
):
    rows, cols = obst_ref.shape
    tiles = cols // LANES
    me = (lax.axis_index("gx"), lax.axis_index("gy"))

    def exists(dx, dy):
        gx, gy = me[0] + dx, me[1] + dy
        return (gx >= 0) & (gx < peers[0]) & (gy >= 0) & (gy < peers[1])

    barrier = pltpu.get_barrier_semaphore()
    count = jnp.int32(0)
    for dx, dy in DIRECTIONS:
        there = exists(dx, dy)
        count = count + there.astype(jnp.int32)

        @pl.when(there)
        def _():
            pl.semaphore_signal(
                barrier, inc=1, device_id=(me[0] + dx, me[1] + dy),
                device_id_type=pl.DeviceIdType.MESH,
            )

    def source(start, size, tile):
        block = (pl.ds(start, size), pl.ds(tile * LANES, LANES))
        return (1 - obst_ref[block]).astype(jnp.float32) * load_ref[block]

    first = SUB + HALO
    for tile in range(tiles):
        top[tile] = source(0, HALO, tile)
        bot[tile] = source(rows - HALO, HALO, tile)
    lane = lane_iota(HALO)
    group = LANES // HALO
    for pack in range(rows // LANES):
        left = jnp.zeros((HALO, LANES), jnp.float32)
        right = jnp.zeros((HALO, LANES), jnp.float32)
        for b in range(group):
            start = pack * LANES + b * HALO
            here = (lane >= b * HALO) & (lane < (b + 1) * HALO)
            low = source(start, HALO, 0)
            high = source(start, HALO, tiles - 1)
            left = jnp.where(here, pltpu.roll(low, b * HALO, 1) if b else low, left)
            turn = ((b + 1) * HALO) % LANES
            right = jnp.where(here, pltpu.roll(high, turn, 1) if turn else high, right)
        lef[pl.ds(pack * HALO, HALO), :] = left
        rig[pl.ds(pack * HALO, HALO), :] = right

    messages = (
        (top, from_rows.at[0]),
        (bot, from_rows.at[1]),
        (lef, from_cols.at[0]),
        (rig, from_cols.at[1]),
        (top.at[0], from_corners.at[0]),
        (top.at[tiles - 1], from_corners.at[1]),
        (bot.at[0], from_corners.at[2]),
        (bot.at[tiles - 1], from_corners.at[3]),
    )

    def copy(k):
        dx, dy = DIRECTIONS[k]
        return pltpu.make_async_remote_copy(
            src_ref=messages[k][0], dst_ref=messages[k][1],
            send_sem=send_sem.at[k], recv_sem=recv_sem.at[k],
            device_id=(me[0] + dx, me[1] + dy), device_id_type=pl.DeviceIdType.MESH,
        )

    pl.semaphore_wait(barrier, count)
    order = (4, 5, 6, 7, 0, 1, 2, 3)
    for k in order:

        @pl.when(exists(*DIRECTIONS[k]))
        def _():
            copy(k).start()

    wide = rows + 2 * HALO
    for tile in range(tiles + 1):
        out_ref[tile, pl.ds(0, SUB), :] = jnp.zeros((SUB, LANES), jnp.float32)
        out_ref[tile, pl.ds(SUB + wide, SUB), :] = jnp.zeros((SUB, LANES), jnp.float32)
    for tile in range(tiles):
        out_ref[tile, pl.ds(first, rows), :] = source(0, rows, tile)

    for k in order:
        dx, dy = DIRECTIONS[k]

        @pl.when(exists(-dx, -dy))
        def _():
            copy(k).wait_recv()

        @pl.when(jnp.logical_not(exists(-dx, -dy)))
        def _():
            messages[k][1][...] = jnp.zeros(messages[k][1].shape, jnp.float32)

    for tile in range(tiles):
        out_ref[tile, pl.ds(first + rows, HALO), :] = from_rows[0, tile]
        out_ref[tile, pl.ds(SUB, HALO), :] = from_rows[1, tile]

    def rim(right, left):
        return jnp.where(lane < HALO, right, jnp.where(lane >= LANES - HALO, left, 0.0))

    out_ref[tiles, pl.ds(first + rows, HALO), :] = rim(from_corners[0], from_corners[1])
    out_ref[tiles, pl.ds(SUB, HALO), :] = rim(from_corners[2], from_corners[3])
    for pack in range(rows // LANES):
        right = from_cols[0, pl.ds(pack * HALO, HALO), :]
        left = from_cols[1, pl.ds(pack * HALO, HALO), :]
        for b in range(group):
            turn_right = (LANES - b * HALO) % LANES
            turn_left = (LANES - HALO - b * HALO) % LANES
            out_ref[tiles, pl.ds(first + pack * LANES + b * HALO, HALO), :] = rim(
                pltpu.roll(right, turn_right, 1) if turn_right else right,
                pltpu.roll(left, turn_left, 1) if turn_left else left,
            )

    for k in order:

        @pl.when(exists(*DIRECTIONS[k]))
        def _():
            copy(k).wait_send()


def cycles_kernel(
    peers, source_ref, exit_rows_ref, exit_cols_ref, out_ref,
    open_ref, marks_ref, diag_ref, first_ref, second_ref, rest_ref, shift_ref,
    expand_ref, corr_ref, fixed_ref, last_ref,
):
    goals, rows, cols = out_ref.shape
    tiles = cols // LANES
    span = tiles + 1
    ring = span * LANES
    wide = rows + 2 * HALO
    groups = wide // SUB
    coarse_rows = wide // COARSEN
    row_start = lax.axis_index("gx") * rows
    col_start = lax.axis_index("gy") * cols
    lane = lane_iota(SUB)
    sub = lax.broadcasted_iota(jnp.int32, (SUB, LANES), 0)
    coefficients = smoother_coefficients()
    inverse = 1.0 / CENTER

    def beside(center):
        up = [pltpu.roll(c, 1, 1) for c in center]
        down = [pltpu.roll(c, LANES - 1, 1) for c in center]
        return [
            jnp.where(lane == 0, up[t - 1], up[t])
            + jnp.where(lane == LANES - 1, down[(t + 1) % len(center)], down[t])
            for t in range(len(center))
        ]

    def load(ref, at, *lead):
        return [ref[(*lead, t, pl.ds(at, SUB), slice(None))] for t in range(span)]

    def cross(ref, at, *lead):
        center = load(ref, at, *lead)
        below = load(ref, at + 1, *lead)
        above = load(ref, at - 1, *lead)
        side = beside(center)
        return center, [below[t] + above[t] + side[t] for t in range(span)]

    def loop(low, high):
        def run(body):
            def step(i, carry):
                body(i, pl.multiple_of(i * SUB + SUB, SUB))
                return carry

            lax.fori_loop(low, high, step, 0)

        return run

    zero = jnp.zeros((SUB, LANES), jnp.float32)
    for ends in (0, wide + SUB):
        for t in range(span):
            open_ref[t, pl.ds(ends, SUB), :] = zero
            corr_ref[t, pl.ds(ends, SUB), :] = zero
            for g in range(goals):
                for ref in (first_ref, second_ref):
                    ref[g, t, pl.ds(ends, SUB), :] = zero

    @loop(0, groups)
    def _(i, at):
        for t in range(span):
            open_ref[t, pl.ds(at, SUB), :] = (source_ref[t, pl.ds(at, SUB), :] > 0.0).astype(
                jnp.float32
            )

    count = exit_rows_ref.shape[1]
    row_of = lax.broadcasted_iota(jnp.int32, (wide, count), 0) + (row_start - HALO)
    ring_lane = lax.broadcasted_iota(jnp.int32, (ring, count), 0)
    col_of = jnp.where(ring_lane < cols + LANES // 2, ring_lane, ring_lane - ring) + col_start
    for g in range(goals):
        row_hot = (row_of == exit_rows_ref[pl.ds(g, 1), :]).astype(jnp.float32)
        col_hot = (col_of == exit_cols_ref[pl.ds(g, 1), :]).astype(jnp.float32)
        marks = lax.dot_general(
            row_hot.astype(jnp.bfloat16), col_hot.astype(jnp.bfloat16),
            (((1,), (1,)), ((), ())), preferred_element_type=jnp.float32,
        )
        for t in range(span):
            marks_ref[g, t] = marks[:, t * LANES : (t + 1) * LANES]

    fine = lax.broadcasted_iota(jnp.int32, (ring, LANES), 0)
    fine = jnp.where(fine < cols + LANES // 2, fine, fine - ring + COARSEN * LANES) // COARSEN
    belongs = (fine == lax.broadcasted_iota(jnp.int32, (ring, LANES), 1)).astype(jnp.float32)

    def restrict(ref, offset, *lead):
        total = None
        for t in range(span):
            block = ref[(*lead, t, pl.ds(offset, coarse_rows, stride=COARSEN), slice(None))]
            for k in range(1, COARSEN):
                block = block + ref[
                    (*lead, t, pl.ds(offset + k, coarse_rows, stride=COARSEN), slice(None))
                ]
            part = lax.dot_general(
                block, belongs[t * LANES : (t + 1) * LANES], (((1,), (0,)), ((), ())),
                precision=lax.Precision.HIGHEST, preferred_element_type=jnp.float32,
            )
            total = part if total is None else total + part
        return total * (1.0 / (COARSEN * COARSEN))

    shape = (coarse_rows, LANES)
    coarse_row = lax.broadcasted_iota(jnp.int32, shape, 0) - COARSE_HALO + row_start // COARSEN
    coarse_lane = lax.broadcasted_iota(jnp.int32, shape, 1)
    coarse_col = (
        jnp.where(coarse_lane < cols // COARSEN + LANES // 8, coarse_lane, coarse_lane - LANES)
        + col_start // COARSEN
    )
    floor = (
        (coarse_row >= 0) & (coarse_row < peers[0] * rows // COARSEN)
        & (coarse_col >= 0) & (coarse_col < peers[1] * cols // COARSEN)
    ).astype(jnp.float32)

    def coarse_solve(rhs):
        center_weight = 4.0 + COARSE_SHIFT
        gain = DAMPING / center_weight
        estimate = gain * rhs * floor
        for sweep in range(CSWEEPS - 1):
            around = (
                pltpu.roll(estimate, coarse_rows - 1, 0) + pltpu.roll(estimate, 1, 0)
                + pltpu.roll(estimate, LANES - 1, 1) + pltpu.roll(estimate, 1, 1)
            )
            estimate = ((1.0 - DAMPING) * estimate + gain * (rhs + around)) * floor
        return estimate

    def widen(estimate, t):
        return lax.dot_general(
            estimate, belongs[t * LANES : (t + 1) * LANES], (((1,), (1,)), ((), ())),
            precision=lax.Precision.HIGHEST, preferred_element_type=jnp.float32,
        )

    def spread(ref, i, t, *lead):
        even = jnp.broadcast_to(ref[(*lead, t, pl.ds(2 * i, 1), slice(None))], (SUB, LANES))
        odd = jnp.broadcast_to(ref[(*lead, t, pl.ds(2 * i + 1, 1), slice(None))], (SUB, LANES))
        return jnp.where(sub < COARSEN, even, odd)

    estimate = coarse_solve(restrict(source_ref, SUB))
    for t in range(span):
        expand_ref[t] = widen(estimate, t)

    @loop(0, groups)
    def _(i, at):
        opened, around = cross(open_ref, at)
        source, source_around = cross(source_ref, at)
        for t in range(span):
            base = SCREENING + 4.0 * (1.0 - opened[t]) + opened[t] * around[t]
            mixed = (coefficients[3] * inverse) * opened[t] * source_around[t]
            mixed = mixed + coefficients[2] * source[t]
            lifted = coefficients[3] * source[t]
            sink = EXIT_SINK * opened[t]
            corr_ref[t, pl.ds(at, SUB), :] = opened[t] * spread(expand_ref, i, t)
            for g in range(goals):
                exits = jnp.minimum(marks_ref[g, t, pl.ds(i * SUB, SUB), :], 1.0)
                kept = 1.0 - (base + sink * exits) * inverse
                diag_ref[g, t, pl.ds(at, SUB), :] = kept
                first_ref[g, t, pl.ds(at, SUB), :] = kept * lifted + mixed

    def horner(old_ref, new_ref, coefficient, rhs):
        def body(i, at):
            weight = [inverse * open_ref[t, pl.ds(at, SUB), :] for t in range(span)]
            for g in range(goals):
                center, around = cross(old_ref, at, g)
                for t in range(span):
                    kept = diag_ref[g, t, pl.ds(at, SUB), :]
                    new_ref[g, t, pl.ds(at, SUB), :] = (
                        kept * center[t] + weight[t] * around[t] + coefficient * rhs(g, t, at)
                    )

        return body

    plain = lambda g, t, at: source_ref[t, pl.ds(at, SUB), :]
    loop(0, groups)(horner(first_ref, second_ref, coefficients[1], plain))
    loop(0, groups)(horner(second_ref, first_ref, coefficients[0], plain))

    @loop(0, groups)
    def _(i, at):
        correction, around_corr = cross(corr_ref, at)
        opened = load(open_ref, at)
        for g in range(goals):
            center, around = cross(first_ref, at, g)
            for t in range(span):
                kept = CENTER * (diag_ref[g, t, pl.ds(at, SUB), :] - 1.0)
                residual = (
                    source_ref[t, pl.ds(at, SUB), :] + kept * center[t] + opened[t] * around[t]
                )
                rest_ref[g, t, pl.ds(i * SUB, SUB), :] = residual
                shift_ref[g, t, pl.ds(at, SUB), :] = (
                    residual + kept * correction[t] + opened[t] * around_corr[t]
                )

    for g in range(goals):
        estimate = coarse_solve(restrict(rest_ref, 0, g))
        for t in range(tiles):
            last_ref[g, t] = widen(estimate, t)

    edge = HALO // SUB

    @loop(edge - 1, groups - edge + 1)
    def _(i, at):
        weight = [(coefficients[3] * inverse) * open_ref[t, pl.ds(at, SUB), :] for t in range(span)]
        for g in range(goals):
            center, around = cross(shift_ref, at, g)
            for t in range(span):
                kept = diag_ref[g, t, pl.ds(at, SUB), :]
                second_ref[g, t, pl.ds(at, SUB), :] = (
                    (coefficients[3] * kept + coefficients[2]) * center[t] + weight[t] * around[t]
                )

    shifted = lambda g, t, at: shift_ref[g, t, pl.ds(at, SUB), :]
    loop(edge - 1, groups - edge + 1)(horner(second_ref, fixed_ref, coefficients[1], shifted))

    @loop(edge, groups - edge)
    def _(i, at):
        opened = load(open_ref, at)
        for g in range(goals):
            center, around = cross(fixed_ref, at, g)
            for t in range(tiles):
                kept = diag_ref[g, t, pl.ds(at, SUB), :]
                smooth = (
                    kept * center[t] + (inverse * opened[t]) * around[t]
                    + coefficients[0] * shift_ref[g, t, pl.ds(at, SUB), :]
                )
                out_ref[g, pl.ds(pl.multiple_of(at - SUB - HALO, SUB), SUB), pl.ds(t * LANES, LANES)] = (
                    first_ref[g, t, pl.ds(at, SUB), :] + corr_ref[t, pl.ds(at, SUB), :]
                    + smooth + opened[t] * spread(last_ref, i, t, g)
                )


def per_device(peers, obstacles, load, exit_rows, exit_cols):
    rows, cols = obstacles.shape
    goals = exit_rows.shape[0]
    tiles = cols // LANES
    span = tiles + 1
    wide = rows + 2 * HALO
    padded = wide + 2 * SUB
    f32 = jnp.float32
    vmem = pl.BlockSpec(memory_space=pltpu.VMEM)
    packed = rows * HALO // LANES
    source = pl.pallas_call(
        functools.partial(exchange_kernel, peers),
        out_shape=jax.ShapeDtypeStruct((span, padded, LANES), f32),
        in_specs=[vmem] * 2,
        out_specs=vmem,
        scratch_shapes=[
            pltpu.VMEM((tiles, HALO, LANES), f32),
            pltpu.VMEM((tiles, HALO, LANES), f32),
            pltpu.VMEM((packed, LANES), f32),
            pltpu.VMEM((packed, LANES), f32),
            pltpu.VMEM((2, tiles, HALO, LANES), f32),
            pltpu.VMEM((2, packed, LANES), f32),
            pltpu.VMEM((4, HALO, LANES), f32),
            pltpu.SemaphoreType.DMA((len(DIRECTIONS),)),
            pltpu.SemaphoreType.DMA((len(DIRECTIONS),)),
        ],
        compiler_params=pltpu.CompilerParams(collective_id=0, has_side_effects=True),
        name="exchange",
    )(obstacles, load)
    field = pltpu.VMEM((goals, span, padded, LANES), f32)
    flat = pltpu.VMEM((goals, span, wide, LANES), f32)
    shared = pltpu.VMEM((span, padded, LANES), f32)
    coarse = wide // COARSEN
    return pl.pallas_call(
        functools.partial(cycles_kernel, peers),
        out_shape=jax.ShapeDtypeStruct((goals, rows, cols), f32),
        in_specs=[vmem] * 3,
        out_specs=vmem,
        scratch_shapes=[
            shared, flat, field, field, field, flat, field,
            pltpu.VMEM((span, coarse, LANES), f32), shared, field,
            pltpu.VMEM((goals, tiles, coarse, LANES), f32),
        ],
        compiler_params=pltpu.CompilerParams(vmem_limit_bytes=48 * 1024 * 1024),
        name="cycles",
    )(source, exit_rows, exit_cols)


def solution(mesh):
    peers = (mesh.shape["gx"], mesh.shape["gy"])
    return jax.shard_map(
        functools.partial(per_device, peers),
        mesh=mesh,
        in_specs=(P("gx", "gy"), P("gx", "gy"), P(), P()),
        out_specs=P(None, "gx", "gy"),
        check_vma=False,
    )
```

```python
import functools

import jax
import jax.numpy as jnp
from jax import lax
from jax.experimental import pallas as pl
from jax.experimental.pallas import tpu as pltpu
from jax.sharding import PartitionSpec as P

COARSEN = 4
SMOOTH = 4
CSWEEPS = 4

SCREENING = 0.0001
EXIT_SINK = 4.0
COARSE_SHIFT = 0.01
DAMPING = 0.8
UPPER_BOUND = 12.5
LOWER_BOUND = 1.0

CENTER = 0.5 * (UPPER_BOUND + LOWER_BOUND)
LANES = 128
SUB = 8
UNROLL = 4
HALO = COARSEN * CSWEEPS
COARSE_HALO = HALO // COARSEN

DIRECTIONS = ((-1, 0), (1, 0), (0, -1), (0, 1), (-1, -1), (-1, 1), (1, -1), (1, 1))


def smoother_coefficients():
    def add(p, q):
        size = max(len(p), len(q))
        p, q = p + [0.0] * (size - len(p)), q + [0.0] * (size - len(q))
        return [a + b for a, b in zip(p, q)]

    def scale(k, p):
        return [k * a for a in p]

    half_span = 0.5 * (UPPER_BOUND - LOWER_BOUND)
    sigma_ratio = CENTER / half_span
    ratio_old = 1.0 / sigma_ratio
    residual = [1.0]
    update = scale(1.0 / CENTER, residual)
    result = update
    for sweep in range(SMOOTH - 1):
        applied = scale(CENTER, add(update, scale(-1.0, [0.0] + update)))
        residual = add(residual, scale(-1.0, applied))
        ratio_new = 1.0 / (2.0 * sigma_ratio - ratio_old)
        update = add(
            scale(ratio_new * ratio_old, update), scale(2.0 * ratio_new / half_span, residual)
        )
        result = add(result, update)
        ratio_old = ratio_new
    return result


def lane_iota(rows):
    return lax.broadcasted_iota(jnp.int32, (rows, LANES), 1)


def exchange_kernel(
    peers, obst_ref, load_ref, out_ref, top, bot, lef, rig, from_rows, from_cols, from_corners,
    send_sem, recv_sem,
):
    rows, cols = obst_ref.shape
    tiles = cols // LANES
    me = (lax.axis_index("gx"), lax.axis_index("gy"))

    def exists(dx, dy):
        gx, gy = me[0] + dx, me[1] + dy
        return (gx >= 0) & (gx < peers[0]) & (gy >= 0) & (gy < peers[1])

    barrier = pltpu.get_barrier_semaphore()
    count = jnp.int32(0)
    for dx, dy in DIRECTIONS:
        there = exists(dx, dy)
        count = count + there.astype(jnp.int32)

        @pl.when(there)
        def _():
            pl.semaphore_signal(
                barrier, inc=1, device_id=(me[0] + dx, me[1] + dy),
                device_id_type=pl.DeviceIdType.MESH,
            )

    def source(start, size, tile):
        block = (pl.ds(start, size), pl.ds(tile * LANES, LANES))
        return (1 - obst_ref[block]).astype(jnp.float32) * load_ref[block]

    first = SUB + HALO
    for tile in range(tiles):
        top[tile] = source(0, HALO, tile)
        bot[tile] = source(rows - HALO, HALO, tile)
    lane = lane_iota(HALO)
    group = LANES // HALO
    for pack in range(rows // LANES):
        left = jnp.zeros((HALO, LANES), jnp.float32)
        right = jnp.zeros((HALO, LANES), jnp.float32)
        for b in range(group):
            start = pack * LANES + b * HALO
            here = (lane >= b * HALO) & (lane < (b + 1) * HALO)
            low = source(start, HALO, 0)
            high = source(start, HALO, tiles - 1)
            left = jnp.where(here, pltpu.roll(low, b * HALO, 1) if b else low, left)
            turn = ((b + 1) * HALO) % LANES
            right = jnp.where(here, pltpu.roll(high, turn, 1) if turn else high, right)
        lef[pl.ds(pack * HALO, HALO), :] = left
        rig[pl.ds(pack * HALO, HALO), :] = right

    messages = (
        (top, from_rows.at[0]),
        (bot, from_rows.at[1]),
        (lef, from_cols.at[0]),
        (rig, from_cols.at[1]),
        (top.at[0], from_corners.at[0]),
        (top.at[tiles - 1], from_corners.at[1]),
        (bot.at[0], from_corners.at[2]),
        (bot.at[tiles - 1], from_corners.at[3]),
    )

    def copy(k):
        dx, dy = DIRECTIONS[k]
        return pltpu.make_async_remote_copy(
            src_ref=messages[k][0], dst_ref=messages[k][1],
            send_sem=send_sem.at[k], recv_sem=recv_sem.at[k],
            device_id=(me[0] + dx, me[1] + dy), device_id_type=pl.DeviceIdType.MESH,
        )

    pl.semaphore_wait(barrier, count)
    order = (4, 5, 6, 7, 0, 1, 2, 3)
    for k in order:

        @pl.when(exists(*DIRECTIONS[k]))
        def _():
            copy(k).start()

    wide = rows + 2 * HALO
    for tile in range(tiles + 1):
        out_ref[tile, pl.ds(0, SUB), :] = jnp.zeros((SUB, LANES), jnp.float32)
        out_ref[tile, pl.ds(SUB + wide, SUB), :] = jnp.zeros((SUB, LANES), jnp.float32)
    for tile in range(tiles):
        out_ref[tile, pl.ds(first, rows), :] = source(0, rows, tile)

    for k in order:
        dx, dy = DIRECTIONS[k]

        @pl.when(exists(-dx, -dy))
        def _():
            copy(k).wait_recv()

        @pl.when(jnp.logical_not(exists(-dx, -dy)))
        def _():
            messages[k][1][...] = jnp.zeros(messages[k][1].shape, jnp.float32)

    for tile in range(tiles):
        out_ref[tile, pl.ds(first + rows, HALO), :] = from_rows[0, tile]
        out_ref[tile, pl.ds(SUB, HALO), :] = from_rows[1, tile]

    def rim(right, left):
        return jnp.where(lane < HALO, right, jnp.where(lane >= LANES - HALO, left, 0.0))

    out_ref[tiles, pl.ds(first + rows, HALO), :] = rim(from_corners[0], from_corners[1])
    out_ref[tiles, pl.ds(SUB, HALO), :] = rim(from_corners[2], from_corners[3])
    for pack in range(rows // LANES):
        right = from_cols[0, pl.ds(pack * HALO, HALO), :]
        left = from_cols[1, pl.ds(pack * HALO, HALO), :]
        for b in range(group):
            turn_right = (LANES - b * HALO) % LANES
            turn_left = (LANES - HALO - b * HALO) % LANES
            out_ref[tiles, pl.ds(first + pack * LANES + b * HALO, HALO), :] = rim(
                pltpu.roll(right, turn_right, 1) if turn_right else right,
                pltpu.roll(left, turn_left, 1) if turn_left else left,
            )

    for k in order:

        @pl.when(exists(*DIRECTIONS[k]))
        def _():
            copy(k).wait_send()


def cycles_kernel(
    peers, source_ref, exit_rows_ref, exit_cols_ref, out_ref,
    open_ref, marks_ref, diag_ref, first_ref, second_ref, rest_ref, shift_ref,
    expand_ref, corr_ref, fixed_ref, last_ref,
):
    goals, rows, cols = out_ref.shape
    tiles = cols // LANES
    span = tiles + 1
    ring = span * LANES
    wide = rows + 2 * HALO
    groups = wide // SUB
    coarse_rows = wide // COARSEN
    row_start = lax.axis_index("gx") * rows
    col_start = lax.axis_index("gy") * cols
    lane = lane_iota(SUB)
    sub = lax.broadcasted_iota(jnp.int32, (SUB, LANES), 0)
    coefficients = smoother_coefficients()
    inverse = 1.0 / CENTER

    def beside(center):
        up = [pltpu.roll(c, 1, 1) for c in center]
        down = [pltpu.roll(c, LANES - 1, 1) for c in center]
        return [
            jnp.where(lane == 0, up[t - 1], up[t])
            + jnp.where(lane == LANES - 1, down[(t + 1) % len(center)], down[t])
            for t in range(len(center))
        ]

    def load(ref, at, *lead):
        return [ref[(*lead, t, pl.ds(at, SUB), slice(None))] for t in range(span)]

    def cross(ref, at, *lead):
        center = load(ref, at, *lead)
        below = load(ref, at + 1, *lead)
        above = load(ref, at - 1, *lead)
        side = beside(center)
        return center, [below[t] + above[t] + side[t] for t in range(span)]

    def loop(low, high):
        def run(body):
            def step(i, carry):
                body(i, pl.multiple_of(i * SUB + SUB, SUB))
                return carry

            count = high - low
            unroll = max(u for u in range(1, UNROLL + 1) if count % u == 0)
            lax.fori_loop(low, high, step, 0, unroll=unroll)

        return run

    zero = jnp.zeros((SUB, LANES), jnp.float32)
    for ends in (0, wide + SUB):
        for t in range(span):
            open_ref[t, pl.ds(ends, SUB), :] = zero
            corr_ref[t, pl.ds(ends, SUB), :] = zero
            for g in range(goals):
                for ref in (first_ref, second_ref):
                    ref[g, t, pl.ds(ends, SUB), :] = zero

    @loop(0, groups)
    def _(i, at):
        for t in range(span):
            open_ref[t, pl.ds(at, SUB), :] = (source_ref[t, pl.ds(at, SUB), :] > 0.0).astype(
                jnp.float32
            )

    count = exit_rows_ref.shape[1]
    row_of = lax.broadcasted_iota(jnp.int32, (wide, count), 0) + (row_start - HALO)
    ring_lane = lax.broadcasted_iota(jnp.int32, (ring, count), 0)
    col_of = jnp.where(ring_lane < cols + LANES // 2, ring_lane, ring_lane - ring) + col_start
    for g in range(goals):
        row_hot = (row_of == exit_rows_ref[pl.ds(g, 1), :]).astype(jnp.float32)
        col_hot = (col_of == exit_cols_ref[pl.ds(g, 1), :]).astype(jnp.float32)
        marks = lax.dot_general(
            row_hot.astype(jnp.bfloat16), col_hot.astype(jnp.bfloat16),
            (((1,), (1,)), ((), ())), preferred_element_type=jnp.float32,
        )
        for t in range(span):
            marks_ref[g, t] = marks[:, t * LANES : (t + 1) * LANES]

    fine = lax.broadcasted_iota(jnp.int32, (ring, LANES), 0)
    fine = jnp.where(fine < cols + LANES // 2, fine, fine - ring + COARSEN * LANES) // COARSEN
    belongs = (fine == lax.broadcasted_iota(jnp.int32, (ring, LANES), 1)).astype(jnp.float32)

    belongs = belongs.astype(jnp.bfloat16)

    def split(value):
        high = value.astype(jnp.bfloat16)
        low = (value - high.astype(jnp.float32)).astype(jnp.bfloat16)
        return jnp.concatenate([high, low], axis=0)

    def product(value, matrix, dims):
        both = lax.dot_general(
            split(value), matrix, (dims, ((), ())), preferred_element_type=jnp.float32
        )
        size = value.shape[0]
        return both[:size] + both[size:]

    def restrict(ref, offset, leads):
        stacked = []
        for t in range(span):
            blocks = []
            for lead in leads:
                part = [
                    ref[(*lead, t, pl.ds(offset + k, coarse_rows, stride=COARSEN), slice(None))]
                    for k in range(COARSEN)
                ]
                blocks.append((part[0] + part[1]) + (part[2] + part[3]))
            stacked.append(jnp.concatenate(blocks, axis=0) if len(blocks) > 1 else blocks[0])
        total = product(jnp.concatenate(stacked, axis=1), belongs, ((1,), (0,)))
        return total * (1.0 / (COARSEN * COARSEN))

    shape = (coarse_rows, LANES)
    coarse_row = lax.broadcasted_iota(jnp.int32, shape, 0) - COARSE_HALO + row_start // COARSEN
    coarse_lane = lax.broadcasted_iota(jnp.int32, shape, 1)
    coarse_col = (
        jnp.where(coarse_lane < cols // COARSEN + LANES // 8, coarse_lane, coarse_lane - LANES)
        + col_start // COARSEN
    )
    floor = (
        (coarse_row >= 0) & (coarse_row < peers[0] * rows // COARSEN)
        & (coarse_col >= 0) & (coarse_col < peers[1] * cols // COARSEN)
    ).astype(jnp.float32)

    def coarse_solve(rhs):
        center_weight = 4.0 + COARSE_SHIFT
        gain = DAMPING / center_weight
        size = rhs.shape[0]
        inside = jnp.concatenate([floor] * (size // coarse_rows), axis=0)
        estimate = gain * rhs * inside
        for sweep in range(CSWEEPS - 1):
            around = (
                pltpu.roll(estimate, size - 1, 0) + pltpu.roll(estimate, 1, 0)
                + pltpu.roll(estimate, LANES - 1, 1) + pltpu.roll(estimate, 1, 1)
            )
            estimate = ((1.0 - DAMPING) * estimate + gain * (rhs + around)) * inside
        return estimate

    def spread(ref, i, t, *lead):
        even = jnp.broadcast_to(ref[(*lead, t, pl.ds(2 * i, 1), slice(None))], (SUB, LANES))
        odd = jnp.broadcast_to(ref[(*lead, t, pl.ds(2 * i + 1, 1), slice(None))], (SUB, LANES))
        return jnp.where(sub < COARSEN, even, odd)

    fine_columns = product(coarse_solve(restrict(source_ref, SUB, [()])), belongs, ((1,), (1,)))
    for t in range(span):
        expand_ref[t] = fine_columns[:, t * LANES : (t + 1) * LANES]

    @loop(0, groups)
    def _(i, at):
        opened, around = cross(open_ref, at)
        source, source_around = cross(source_ref, at)
        for t in range(span):
            base = SCREENING + 4.0 * (1.0 - opened[t]) + opened[t] * around[t]
            mixed = (coefficients[3] * inverse) * opened[t] * source_around[t]
            mixed = mixed + coefficients[2] * source[t]
            lifted = coefficients[3] * source[t]
            sink = EXIT_SINK * opened[t]
            corr_ref[t, pl.ds(at, SUB), :] = opened[t] * spread(expand_ref, i, t)
            for g in range(goals):
                exits = jnp.minimum(marks_ref[g, t, pl.ds(i * SUB, SUB), :], 1.0)
                kept = 1.0 - (base + sink * exits) * inverse
                diag_ref[g, t, pl.ds(at, SUB), :] = kept
                first_ref[g, t, pl.ds(at, SUB), :] = kept * lifted + mixed

    def horner(old_ref, new_ref, coefficient, rhs):
        def body(i, at):
            weight = [inverse * open_ref[t, pl.ds(at, SUB), :] for t in range(span)]
            for g in range(goals):
                center, around = cross(old_ref, at, g)
                for t in range(span):
                    kept = diag_ref[g, t, pl.ds(at, SUB), :]
                    new_ref[g, t, pl.ds(at, SUB), :] = (
                        kept * center[t] + weight[t] * around[t] + coefficient * rhs(g, t, at)
                    )

        return body

    plain = lambda g, t, at: source_ref[t, pl.ds(at, SUB), :]
    loop(0, groups)(horner(first_ref, second_ref, coefficients[1], plain))
    loop(0, groups)(horner(second_ref, first_ref, coefficients[0], plain))

    @loop(0, groups)
    def _(i, at):
        correction, around_corr = cross(corr_ref, at)
        opened = load(open_ref, at)
        for g in range(goals):
            center, around = cross(first_ref, at, g)
            for t in range(span):
                kept = CENTER * (diag_ref[g, t, pl.ds(at, SUB), :] - 1.0)
                residual = (
                    source_ref[t, pl.ds(at, SUB), :] + kept * center[t] + opened[t] * around[t]
                )
                rest_ref[g, t, pl.ds(i * SUB, SUB), :] = residual
                shift_ref[g, t, pl.ds(at, SUB), :] = (
                    residual + kept * correction[t] + opened[t] * around_corr[t]
                )

    estimates = coarse_solve(restrict(rest_ref, 0, [(g,) for g in range(goals)]))
    fine_columns = product(estimates, belongs[:cols], ((1,), (1,)))
    for g in range(goals):
        for t in range(tiles):
            last_ref[g, t] = fine_columns[
                g * coarse_rows : (g + 1) * coarse_rows, t * LANES : (t + 1) * LANES
            ]

    edge = HALO // SUB

    @loop(edge - 1, groups - edge + 1)
    def _(i, at):
        weight = [(coefficients[3] * inverse) * open_ref[t, pl.ds(at, SUB), :] for t in range(span)]
        for g in range(goals):
            center, around = cross(shift_ref, at, g)
            for t in range(span):
                kept = diag_ref[g, t, pl.ds(at, SUB), :]
                second_ref[g, t, pl.ds(at, SUB), :] = (
                    (coefficients[3] * kept + coefficients[2]) * center[t] + weight[t] * around[t]
                )

    shifted = lambda g, t, at: shift_ref[g, t, pl.ds(at, SUB), :]
    loop(edge - 1, groups - edge + 1)(horner(second_ref, fixed_ref, coefficients[1], shifted))

    @loop(edge, groups - edge)
    def _(i, at):
        opened = load(open_ref, at)
        for g in range(goals):
            center, around = cross(fixed_ref, at, g)
            for t in range(tiles):
                kept = diag_ref[g, t, pl.ds(at, SUB), :]
                smooth = (
                    kept * center[t] + (inverse * opened[t]) * around[t]
                    + coefficients[0] * shift_ref[g, t, pl.ds(at, SUB), :]
                )
                out_ref[g, pl.ds(pl.multiple_of(at - SUB - HALO, SUB), SUB), pl.ds(t * LANES, LANES)] = (
                    first_ref[g, t, pl.ds(at, SUB), :] + corr_ref[t, pl.ds(at, SUB), :]
                    + smooth + opened[t] * spread(last_ref, i, t, g)
                )


def per_device(peers, obstacles, load, exit_rows, exit_cols):
    rows, cols = obstacles.shape
    goals = exit_rows.shape[0]
    tiles = cols // LANES
    span = tiles + 1
    wide = rows + 2 * HALO
    padded = wide + 2 * SUB
    f32 = jnp.float32
    vmem = pl.BlockSpec(memory_space=pltpu.VMEM)
    packed = rows * HALO // LANES
    source = pl.pallas_call(
        functools.partial(exchange_kernel, peers),
        out_shape=jax.ShapeDtypeStruct((span, padded, LANES), f32),
        in_specs=[vmem] * 2,
        out_specs=vmem,
        scratch_shapes=[
            pltpu.VMEM((tiles, HALO, LANES), f32),
            pltpu.VMEM((tiles, HALO, LANES), f32),
            pltpu.VMEM((packed, LANES), f32),
            pltpu.VMEM((packed, LANES), f32),
            pltpu.VMEM((2, tiles, HALO, LANES), f32),
            pltpu.VMEM((2, packed, LANES), f32),
            pltpu.VMEM((4, HALO, LANES), f32),
            pltpu.SemaphoreType.DMA((len(DIRECTIONS),)),
            pltpu.SemaphoreType.DMA((len(DIRECTIONS),)),
        ],
        compiler_params=pltpu.CompilerParams(collective_id=0, has_side_effects=True),
        name="exchange",
    )(obstacles, load)
    field = pltpu.VMEM((goals, span, padded, LANES), f32)
    flat = pltpu.VMEM((goals, span, wide, LANES), f32)
    shared = pltpu.VMEM((span, padded, LANES), f32)
    coarse = wide // COARSEN
    return pl.pallas_call(
        functools.partial(cycles_kernel, peers),
        out_shape=jax.ShapeDtypeStruct((goals, rows, cols), f32),
        in_specs=[vmem] * 3,
        out_specs=vmem,
        scratch_shapes=[
            shared, flat, field, field, field, flat, field,
            pltpu.VMEM((span, coarse, LANES), f32), shared, field,
            pltpu.VMEM((goals, tiles, coarse, LANES), f32),
        ],
        compiler_params=pltpu.CompilerParams(vmem_limit_bytes=48 * 1024 * 1024),
        name="cycles",
    )(source, exit_rows, exit_cols)


def solution(mesh):
    peers = (mesh.shape["gx"], mesh.shape["gy"])
    return jax.shard_map(
        functools.partial(per_device, peers),
        mesh=mesh,
        in_specs=(P("gx", "gy"), P("gx", "gy"), P(), P()),
        out_specs=P(None, "gx", "gy"),
        check_vma=False,
    )
```

```python
import functools

import jax
import jax.numpy as jnp
from jax import lax
from jax.experimental import pallas as pl
from jax.experimental.pallas import tpu as pltpu
from jax.sharding import PartitionSpec as P

COARSEN = 4
SMOOTH = 4
CSWEEPS = 4

SCREENING = 0.0001
EXIT_SINK = 4.0
COARSE_SHIFT = 0.01
DAMPING = 0.8
UPPER_BOUND = 12.5
LOWER_BOUND = 1.0

CENTER = 0.5 * (UPPER_BOUND + LOWER_BOUND)
LANES = 128
SUB = 8
UNROLL = 6
HALO = COARSEN * CSWEEPS
COARSE_HALO = HALO // COARSEN

DIRECTIONS = ((-1, 0), (1, 0), (0, -1), (0, 1), (-1, -1), (-1, 1), (1, -1), (1, 1))


def smoother_coefficients():
    def add(p, q):
        size = max(len(p), len(q))
        p, q = p + [0.0] * (size - len(p)), q + [0.0] * (size - len(q))
        return [a + b for a, b in zip(p, q)]

    def scale(k, p):
        return [k * a for a in p]

    half_span = 0.5 * (UPPER_BOUND - LOWER_BOUND)
    sigma_ratio = CENTER / half_span
    ratio_old = 1.0 / sigma_ratio
    residual = [1.0]
    update = scale(1.0 / CENTER, residual)
    result = update
    for sweep in range(SMOOTH - 1):
        applied = scale(CENTER, add(update, scale(-1.0, [0.0] + update)))
        residual = add(residual, scale(-1.0, applied))
        ratio_new = 1.0 / (2.0 * sigma_ratio - ratio_old)
        update = add(
            scale(ratio_new * ratio_old, update), scale(2.0 * ratio_new / half_span, residual)
        )
        result = add(result, update)
        ratio_old = ratio_new
    return result


def lane_iota(rows):
    return lax.broadcasted_iota(jnp.int32, (rows, LANES), 1)


def exchange(
    peers, inputs, obst_ref, load_ref, out_ref, top, bot, lef, rig, from_rows, from_cols,
    from_corners, send_sem, recv_sem, meanwhile,
):
    rows, cols = obst_ref.shape
    tiles = cols // LANES
    me = (lax.axis_index("gx"), lax.axis_index("gy"))

    def exists(dx, dy):
        gx, gy = me[0] + dx, me[1] + dy
        return (gx >= 0) & (gx < peers[0]) & (gy >= 0) & (gy < peers[1])

    barrier = pltpu.get_barrier_semaphore()
    count = jnp.int32(0)
    for dx, dy in DIRECTIONS:
        there = exists(dx, dy)
        count = count + there.astype(jnp.int32)

        @pl.when(there)
        def _():
            pl.semaphore_signal(
                barrier, inc=1, device_id=(me[0] + dx, me[1] + dy),
                device_id_type=pl.DeviceIdType.MESH,
            )

    for copied in inputs:
        copied.start()
    for copied in inputs:
        copied.wait()

    def source(start, size, tile):
        block = (pl.ds(start, size), pl.ds(tile * LANES, LANES))
        return (1 - obst_ref[block]).astype(jnp.float32) * load_ref[block]

    first = SUB + HALO
    for tile in range(tiles):
        top[tile] = source(0, HALO, tile)
        bot[tile] = source(rows - HALO, HALO, tile)
    lane = lane_iota(HALO)
    group = LANES // HALO
    for pack in range(rows // LANES):
        left = jnp.zeros((HALO, LANES), jnp.float32)
        right = jnp.zeros((HALO, LANES), jnp.float32)
        for b in range(group):
            start = pack * LANES + b * HALO
            here = (lane >= b * HALO) & (lane < (b + 1) * HALO)
            low = source(start, HALO, 0)
            high = source(start, HALO, tiles - 1)
            left = jnp.where(here, pltpu.roll(low, b * HALO, 1) if b else low, left)
            turn = ((b + 1) * HALO) % LANES
            right = jnp.where(here, pltpu.roll(high, turn, 1) if turn else high, right)
        lef[pl.ds(pack * HALO, HALO), :] = left
        rig[pl.ds(pack * HALO, HALO), :] = right

    messages = (
        (top, from_rows.at[0]),
        (bot, from_rows.at[1]),
        (lef, from_cols.at[0]),
        (rig, from_cols.at[1]),
        (top.at[0], from_corners.at[0]),
        (top.at[tiles - 1], from_corners.at[1]),
        (bot.at[0], from_corners.at[2]),
        (bot.at[tiles - 1], from_corners.at[3]),
    )

    def copy(k):
        dx, dy = DIRECTIONS[k]
        return pltpu.make_async_remote_copy(
            src_ref=messages[k][0], dst_ref=messages[k][1],
            send_sem=send_sem.at[k], recv_sem=recv_sem.at[k],
            device_id=(me[0] + dx, me[1] + dy), device_id_type=pl.DeviceIdType.MESH,
        )

    pl.semaphore_wait(barrier, count)
    order = (4, 5, 6, 7, 0, 1, 2, 3)
    for k in order:

        @pl.when(exists(*DIRECTIONS[k]))
        def _():
            copy(k).start()

    wide = rows + 2 * HALO
    for tile in range(tiles + 1):
        out_ref[tile, pl.ds(0, SUB), :] = jnp.zeros((SUB, LANES), jnp.float32)
        out_ref[tile, pl.ds(SUB + wide, SUB), :] = jnp.zeros((SUB, LANES), jnp.float32)
    for tile in range(tiles):
        out_ref[tile, pl.ds(first, rows), :] = source(0, rows, tile)

    meanwhile()

    for k in order:
        dx, dy = DIRECTIONS[k]

        @pl.when(exists(-dx, -dy))
        def _():
            copy(k).wait_recv()

        @pl.when(jnp.logical_not(exists(-dx, -dy)))
        def _():
            messages[k][1][...] = jnp.zeros(messages[k][1].shape, jnp.float32)

    for tile in range(tiles):
        out_ref[tile, pl.ds(first + rows, HALO), :] = from_rows[0, tile]
        out_ref[tile, pl.ds(SUB, HALO), :] = from_rows[1, tile]

    def rim(right, left):
        return jnp.where(lane < HALO, right, jnp.where(lane >= LANES - HALO, left, 0.0))

    out_ref[tiles, pl.ds(first + rows, HALO), :] = rim(from_corners[0], from_corners[1])
    out_ref[tiles, pl.ds(SUB, HALO), :] = rim(from_corners[2], from_corners[3])
    for pack in range(rows // LANES):
        right = from_cols[0, pl.ds(pack * HALO, HALO), :]
        left = from_cols[1, pl.ds(pack * HALO, HALO), :]
        for b in range(group):
            turn_right = (LANES - b * HALO) % LANES
            turn_left = (LANES - HALO - b * HALO) % LANES
            out_ref[tiles, pl.ds(first + pack * LANES + b * HALO, HALO), :] = rim(
                pltpu.roll(right, turn_right, 1) if turn_right else right,
                pltpu.roll(left, turn_left, 1) if turn_left else left,
            )

    for k in order:

        @pl.when(exists(*DIRECTIONS[k]))
        def _():
            copy(k).wait_send()


def cycles_kernel(
    peers, obst_hbm, load_hbm, rows_hbm, cols_hbm, out_ref,
    obst_ref, load_ref, exit_rows_ref, exit_cols_ref, source_ref,
    open_ref, marks_ref, diag_ref, first_ref, second_ref, rest_ref, shift_ref,
    expand_ref, corr_ref, fixed_ref, last_ref,
    top, bot, lef, rig, from_rows, from_cols, from_corners, input_sem, send_sem, recv_sem,
):
    goals, rows, cols = out_ref.shape
    tiles = cols // LANES
    span = tiles + 1
    ring = span * LANES
    wide = rows + 2 * HALO
    groups = wide // SUB
    coarse_rows = wide // COARSEN
    row_start = lax.axis_index("gx") * rows
    col_start = lax.axis_index("gy") * cols
    lane = lane_iota(SUB)
    sub = lax.broadcasted_iota(jnp.int32, (SUB, LANES), 0)
    coefficients = smoother_coefficients()
    inverse = 1.0 / CENTER

    def beside(center):
        up = [pltpu.roll(c, 1, 1) for c in center]
        down = [pltpu.roll(c, LANES - 1, 1) for c in center]
        return [
            jnp.where(lane == 0, up[t - 1], up[t])
            + jnp.where(lane == LANES - 1, down[(t + 1) % len(center)], down[t])
            for t in range(len(center))
        ]

    def load(ref, at, *lead):
        return [ref[(*lead, t, pl.ds(at, SUB), slice(None))] for t in range(span)]

    def cross(ref, at, *lead):
        center = load(ref, at, *lead)
        below = load(ref, at + 1, *lead)
        above = load(ref, at - 1, *lead)
        side = beside(center)
        return center, [below[t] + above[t] + side[t] for t in range(span)]

    def loop(low, high):
        def run(body):
            def step(i, carry):
                body(i, pl.multiple_of(i * SUB + SUB, SUB))
                return carry

            count = high - low
            unroll = max(u for u in range(1, UNROLL + 1) if count % u == 0)
            lax.fori_loop(low, high, step, 0, unroll=unroll)

        return run

    def meanwhile():
        zero = jnp.zeros((SUB, LANES), jnp.float32)
        for ends in (0, wide + SUB):
            for t in range(span):
                open_ref[t, pl.ds(ends, SUB), :] = zero
                corr_ref[t, pl.ds(ends, SUB), :] = zero
                for g in range(goals):
                    for ref in (first_ref, second_ref):
                        ref[g, t, pl.ds(ends, SUB), :] = zero

        count = exit_rows_ref.shape[1]
        row_of = lax.broadcasted_iota(jnp.int32, (wide, count), 0) + (row_start - HALO)
        ring_lane = lax.broadcasted_iota(jnp.int32, (ring, count), 0)
        col_of = jnp.where(ring_lane < cols + LANES // 2, ring_lane, ring_lane - ring) + col_start
        for g in range(goals):
            row_hot = (row_of == exit_rows_ref[pl.ds(g, 1), :]).astype(jnp.float32)
            col_hot = (col_of == exit_cols_ref[pl.ds(g, 1), :]).astype(jnp.float32)
            marks = lax.dot_general(
                row_hot.astype(jnp.bfloat16), col_hot.astype(jnp.bfloat16),
                (((1,), (1,)), ((), ())), preferred_element_type=jnp.float32,
            )
            for t in range(span):
                marks_ref[g, t] = marks[:, t * LANES : (t + 1) * LANES]

    pairs = (
        (obst_hbm, obst_ref), (load_hbm, load_ref), (rows_hbm, exit_rows_ref),
        (cols_hbm, exit_cols_ref),
    )
    inputs = [
        pltpu.make_async_copy(there, here, input_sem.at[k]) for k, (there, here) in enumerate(pairs)
    ]
    exchange(
        peers, inputs, obst_ref, load_ref, source_ref, top, bot, lef, rig, from_rows, from_cols,
        from_corners, send_sem, recv_sem, meanwhile,
    )

    @loop(0, groups)
    def _(i, at):
        for t in range(span):
            open_ref[t, pl.ds(at, SUB), :] = (source_ref[t, pl.ds(at, SUB), :] > 0.0).astype(
                jnp.float32
            )

    fine = lax.broadcasted_iota(jnp.int32, (ring, LANES), 0)
    fine = jnp.where(fine < cols + LANES // 2, fine, fine - ring + COARSEN * LANES) // COARSEN
    belongs = (fine == lax.broadcasted_iota(jnp.int32, (ring, LANES), 1)).astype(jnp.float32)

    belongs = belongs.astype(jnp.bfloat16)

    def split(value):
        high = value.astype(jnp.bfloat16)
        low = (value - high.astype(jnp.float32)).astype(jnp.bfloat16)
        return jnp.concatenate([high, low], axis=0)

    def product(value, matrix, dims):
        both = lax.dot_general(
            split(value), matrix, (dims, ((), ())), preferred_element_type=jnp.float32
        )
        size = value.shape[0]
        return both[:size] + both[size:]

    def restrict(ref, offset, leads):
        stacked = []
        for t in range(span):
            blocks = []
            for lead in leads:
                part = [
                    ref[(*lead, t, pl.ds(offset + k, coarse_rows, stride=COARSEN), slice(None))]
                    for k in range(COARSEN)
                ]
                blocks.append((part[0] + part[1]) + (part[2] + part[3]))
            stacked.append(jnp.concatenate(blocks, axis=0) if len(blocks) > 1 else blocks[0])
        total = product(jnp.concatenate(stacked, axis=1), belongs, ((1,), (0,)))
        return total * (1.0 / (COARSEN * COARSEN))

    shape = (coarse_rows, LANES)
    coarse_row = lax.broadcasted_iota(jnp.int32, shape, 0) - COARSE_HALO + row_start // COARSEN
    coarse_lane = lax.broadcasted_iota(jnp.int32, shape, 1)
    coarse_col = (
        jnp.where(coarse_lane < cols // COARSEN + LANES // 8, coarse_lane, coarse_lane - LANES)
        + col_start // COARSEN
    )
    floor = (
        (coarse_row >= 0) & (coarse_row < peers[0] * rows // COARSEN)
        & (coarse_col >= 0) & (coarse_col < peers[1] * cols // COARSEN)
    ).astype(jnp.float32)

    def coarse_solve(rhs):
        center_weight = 4.0 + COARSE_SHIFT
        gain = DAMPING / center_weight
        size = rhs.shape[0]
        inside = jnp.concatenate([floor] * (size // coarse_rows), axis=0)
        estimate = gain * rhs * inside
        for sweep in range(CSWEEPS - 1):
            around = (
                pltpu.roll(estimate, size - 1, 0) + pltpu.roll(estimate, 1, 0)
                + pltpu.roll(estimate, LANES - 1, 1) + pltpu.roll(estimate, 1, 1)
            )
            estimate = ((1.0 - DAMPING) * estimate + gain * (rhs + around)) * inside
        return estimate

    def spread(ref, i, t, *lead):
        even = jnp.broadcast_to(ref[(*lead, t, pl.ds(2 * i, 1), slice(None))], (SUB, LANES))
        odd = jnp.broadcast_to(ref[(*lead, t, pl.ds(2 * i + 1, 1), slice(None))], (SUB, LANES))
        return jnp.where(sub < COARSEN, even, odd)

    fine_columns = product(coarse_solve(restrict(source_ref, SUB, [()])), belongs, ((1,), (1,)))
    for t in range(span):
        expand_ref[t] = fine_columns[:, t * LANES : (t + 1) * LANES]

    @loop(0, groups)
    def _(i, at):
        opened, around = cross(open_ref, at)
        source, source_around = cross(source_ref, at)
        for t in range(span):
            base = SCREENING + 4.0 * (1.0 - opened[t]) + opened[t] * around[t]
            mixed = (coefficients[3] * inverse) * opened[t] * source_around[t]
            mixed = mixed + coefficients[2] * source[t]
            lifted = coefficients[3] * source[t]
            sink = EXIT_SINK * opened[t]
            corr_ref[t, pl.ds(at, SUB), :] = opened[t] * spread(expand_ref, i, t)
            for g in range(goals):
                exits = jnp.minimum(marks_ref[g, t, pl.ds(i * SUB, SUB), :], 1.0)
                kept = 1.0 - (base + sink * exits) * inverse
                diag_ref[g, t, pl.ds(at, SUB), :] = kept
                first_ref[g, t, pl.ds(at, SUB), :] = kept * lifted + mixed

    def horner(old_ref, new_ref, coefficient, rhs):
        def body(i, at):
            weight = [inverse * open_ref[t, pl.ds(at, SUB), :] for t in range(span)]
            for g in range(goals):
                center, around = cross(old_ref, at, g)
                for t in range(span):
                    kept = diag_ref[g, t, pl.ds(at, SUB), :]
                    new_ref[g, t, pl.ds(at, SUB), :] = (
                        kept * center[t] + weight[t] * around[t] + coefficient * rhs(g, t, at)
                    )

        return body

    plain = lambda g, t, at: source_ref[t, pl.ds(at, SUB), :]
    loop(0, groups)(horner(first_ref, second_ref, coefficients[1], plain))
    loop(0, groups)(horner(second_ref, first_ref, coefficients[0], plain))

    @loop(0, groups)
    def _(i, at):
        correction, around_corr = cross(corr_ref, at)
        opened = load(open_ref, at)
        for g in range(goals):
            center, around = cross(first_ref, at, g)
            for t in range(span):
                kept = CENTER * (diag_ref[g, t, pl.ds(at, SUB), :] - 1.0)
                residual = (
                    source_ref[t, pl.ds(at, SUB), :] + kept * center[t] + opened[t] * around[t]
                )
                rest_ref[g, t, pl.ds(i * SUB, SUB), :] = residual
                shift_ref[g, t, pl.ds(at, SUB), :] = (
                    residual + kept * correction[t] + opened[t] * around_corr[t]
                )

    estimates = coarse_solve(restrict(rest_ref, 0, [(g,) for g in range(goals)]))
    fine_columns = product(estimates, belongs[:cols], ((1,), (1,)))
    for g in range(goals):
        for t in range(tiles):
            last_ref[g, t] = fine_columns[
                g * coarse_rows : (g + 1) * coarse_rows, t * LANES : (t + 1) * LANES
            ]

    edge = HALO // SUB

    @loop(edge - 1, groups - edge + 1)
    def _(i, at):
        weight = [(coefficients[3] * inverse) * open_ref[t, pl.ds(at, SUB), :] for t in range(span)]
        for g in range(goals):
            center, around = cross(shift_ref, at, g)
            for t in range(span):
                kept = diag_ref[g, t, pl.ds(at, SUB), :]
                second_ref[g, t, pl.ds(at, SUB), :] = (
                    (coefficients[3] * kept + coefficients[2]) * center[t] + weight[t] * around[t]
                )

    shifted = lambda g, t, at: shift_ref[g, t, pl.ds(at, SUB), :]
    loop(edge - 1, groups - edge + 1)(horner(second_ref, fixed_ref, coefficients[1], shifted))

    @loop(edge, groups - edge)
    def _(i, at):
        opened = load(open_ref, at)
        for g in range(goals):
            center, around = cross(fixed_ref, at, g)
            for t in range(tiles):
                kept = diag_ref[g, t, pl.ds(at, SUB), :]
                smooth = (
                    kept * center[t] + (inverse * opened[t]) * around[t]
                    + coefficients[0] * shift_ref[g, t, pl.ds(at, SUB), :]
                )
                out_ref[g, pl.ds(pl.multiple_of(at - SUB - HALO, SUB), SUB), pl.ds(t * LANES, LANES)] = (
                    first_ref[g, t, pl.ds(at, SUB), :] + corr_ref[t, pl.ds(at, SUB), :]
                    + smooth + opened[t] * spread(last_ref, i, t, g)
                )


def per_device(peers, obstacles, load, exit_rows, exit_cols):
    rows, cols = obstacles.shape
    goals = exit_rows.shape[0]
    tiles = cols // LANES
    span = tiles + 1
    wide = rows + 2 * HALO
    padded = wide + 2 * SUB
    f32 = jnp.float32
    vmem = pl.BlockSpec(memory_space=pltpu.VMEM)
    packed = rows * HALO // LANES
    exits = exit_rows.shape
    field = pltpu.VMEM((goals, span, padded, LANES), f32)
    flat = pltpu.VMEM((goals, span, wide, LANES), f32)
    shared = pltpu.VMEM((span, padded, LANES), f32)
    coarse = wide // COARSEN
    return pl.pallas_call(
        functools.partial(cycles_kernel, peers),
        out_shape=jax.ShapeDtypeStruct((goals, rows, cols), f32),
        in_specs=[pl.BlockSpec(memory_space=pltpu.HBM)] * 4,
        out_specs=vmem,
        scratch_shapes=[
            pltpu.VMEM((rows, cols), jnp.int32),
            pltpu.VMEM((rows, cols), f32),
            pltpu.VMEM(exits, jnp.int32),
            pltpu.VMEM(exits, jnp.int32),
            shared,
            shared, flat, field, field, field, flat, field,
            pltpu.VMEM((span, coarse, LANES), f32), shared, field,
            pltpu.VMEM((goals, tiles, coarse, LANES), f32),
            pltpu.VMEM((tiles, HALO, LANES), f32),
            pltpu.VMEM((tiles, HALO, LANES), f32),
            pltpu.VMEM((packed, LANES), f32),
            pltpu.VMEM((packed, LANES), f32),
            pltpu.VMEM((2, tiles, HALO, LANES), f32),
            pltpu.VMEM((2, packed, LANES), f32),
            pltpu.VMEM((4, HALO, LANES), f32),
            pltpu.SemaphoreType.DMA((4,)),
            pltpu.SemaphoreType.DMA((len(DIRECTIONS),)),
            pltpu.SemaphoreType.DMA((len(DIRECTIONS),)),
        ],
        compiler_params=pltpu.CompilerParams(
            collective_id=0, has_side_effects=True, vmem_limit_bytes=48 * 1024 * 1024
        ),
        name="cycles",
    )(*(pltpu.with_memory_space_constraint(x, pltpu.HBM) for x in (obstacles, load, exit_rows, exit_cols)))


def solution(mesh):
    peers = (mesh.shape["gx"], mesh.shape["gy"])
    return jax.shard_map(
        functools.partial(per_device, peers),
        mesh=mesh,
        in_specs=(P("gx", "gy"), P("gx", "gy"), P(), P()),
        out_specs=P(None, "gx", "gy"),
        check_vma=False,
    )
```

```python
import functools

import jax
import jax.numpy as jnp
from jax import lax
from jax.experimental import pallas as pl
from jax.experimental.pallas import tpu as pltpu
from jax.sharding import PartitionSpec as P

COARSEN = 4
SMOOTH = 4
CSWEEPS = 4

SCREENING = 0.0001
EXIT_SINK = 4.0
COARSE_SHIFT = 0.01
DAMPING = 0.8
UPPER_BOUND = 12.5
LOWER_BOUND = 1.0

CENTER = 0.5 * (UPPER_BOUND + LOWER_BOUND)
LANES = 128
SUB = 8
UNROLL = 10
HALO = COARSEN * CSWEEPS
COARSE_HALO = HALO // COARSEN

DIRECTIONS = ((-1, 0), (1, 0), (0, -1), (0, 1), (-1, -1), (-1, 1), (1, -1), (1, 1))


def smoother_coefficients():
    def add(p, q):
        size = max(len(p), len(q))
        p, q = p + [0.0] * (size - len(p)), q + [0.0] * (size - len(q))
        return [a + b for a, b in zip(p, q)]

    def scale(k, p):
        return [k * a for a in p]

    half_span = 0.5 * (UPPER_BOUND - LOWER_BOUND)
    sigma_ratio = CENTER / half_span
    ratio_old = 1.0 / sigma_ratio
    residual = [1.0]
    update = scale(1.0 / CENTER, residual)
    result = update
    for sweep in range(SMOOTH - 1):
        applied = scale(CENTER, add(update, scale(-1.0, [0.0] + update)))
        residual = add(residual, scale(-1.0, applied))
        ratio_new = 1.0 / (2.0 * sigma_ratio - ratio_old)
        update = add(
            scale(ratio_new * ratio_old, update), scale(2.0 * ratio_new / half_span, residual)
        )
        result = add(result, update)
        ratio_old = ratio_new
    return result


def lane_iota(rows):
    return lax.broadcasted_iota(jnp.int32, (rows, LANES), 1)


def exchange(
    peers, inputs, obst_ref, load_ref, out_ref, top, bot, lef, rig, from_rows, from_cols,
    from_corners, send_sem, recv_sem, meanwhile,
):
    rows, cols = obst_ref.shape
    tiles = cols // LANES
    me = (lax.axis_index("gx"), lax.axis_index("gy"))

    def exists(dx, dy):
        gx, gy = me[0] + dx, me[1] + dy
        return (gx >= 0) & (gx < peers[0]) & (gy >= 0) & (gy < peers[1])

    barrier = pltpu.get_barrier_semaphore()
    count = jnp.int32(0)
    for dx, dy in DIRECTIONS:
        there = exists(dx, dy)
        count = count + there.astype(jnp.int32)

        @pl.when(there)
        def _():
            pl.semaphore_signal(
                barrier, inc=1, device_id=(me[0] + dx, me[1] + dy),
                device_id_type=pl.DeviceIdType.MESH,
            )

    for copied in inputs:
        copied.start()
    for copied in inputs:
        copied.wait()

    def source(start, size, tile):
        block = (pl.ds(start, size), pl.ds(tile * LANES, LANES))
        return (1 - obst_ref[block]).astype(jnp.float32) * load_ref[block]

    first = SUB + HALO
    for tile in range(tiles):
        top[tile] = source(0, HALO, tile)
        bot[tile] = source(rows - HALO, HALO, tile)
    lane = lane_iota(HALO)
    group = LANES // HALO
    for pack in range(rows // LANES):
        left = jnp.zeros((HALO, LANES), jnp.float32)
        right = jnp.zeros((HALO, LANES), jnp.float32)
        for b in range(group):
            start = pack * LANES + b * HALO
            here = (lane >= b * HALO) & (lane < (b + 1) * HALO)
            low = source(start, HALO, 0)
            high = source(start, HALO, tiles - 1)
            left = jnp.where(here, pltpu.roll(low, b * HALO, 1) if b else low, left)
            turn = ((b + 1) * HALO) % LANES
            right = jnp.where(here, pltpu.roll(high, turn, 1) if turn else high, right)
        lef[pl.ds(pack * HALO, HALO), :] = left
        rig[pl.ds(pack * HALO, HALO), :] = right

    messages = (
        (top, from_rows.at[0]),
        (bot, from_rows.at[1]),
        (lef, from_cols.at[0]),
        (rig, from_cols.at[1]),
        (top.at[0], from_corners.at[0]),
        (top.at[tiles - 1], from_corners.at[1]),
        (bot.at[0], from_corners.at[2]),
        (bot.at[tiles - 1], from_corners.at[3]),
    )

    def copy(k):
        dx, dy = DIRECTIONS[k]
        return pltpu.make_async_remote_copy(
            src_ref=messages[k][0], dst_ref=messages[k][1],
            send_sem=send_sem.at[k], recv_sem=recv_sem.at[k],
            device_id=(me[0] + dx, me[1] + dy), device_id_type=pl.DeviceIdType.MESH,
        )

    pl.semaphore_wait(barrier, count)
    order = (4, 5, 6, 7, 0, 1, 2, 3)
    for k in order:

        @pl.when(exists(*DIRECTIONS[k]))
        def _():
            copy(k).start()

    wide = rows + 2 * HALO
    for tile in range(tiles + 1):
        out_ref[tile, pl.ds(0, SUB), :] = jnp.zeros((SUB, LANES), jnp.float32)
        out_ref[tile, pl.ds(SUB + wide, SUB), :] = jnp.zeros((SUB, LANES), jnp.float32)
    for tile in range(tiles):
        out_ref[tile, pl.ds(first, rows), :] = source(0, rows, tile)

    meanwhile()

    for k in order:
        dx, dy = DIRECTIONS[k]

        @pl.when(exists(-dx, -dy))
        def _():
            copy(k).wait_recv()

        @pl.when(jnp.logical_not(exists(-dx, -dy)))
        def _():
            messages[k][1][...] = jnp.zeros(messages[k][1].shape, jnp.float32)

    for tile in range(tiles):
        out_ref[tile, pl.ds(first + rows, HALO), :] = from_rows[0, tile]
        out_ref[tile, pl.ds(SUB, HALO), :] = from_rows[1, tile]

    def rim(right, left):
        return jnp.where(lane < HALO, right, jnp.where(lane >= LANES - HALO, left, 0.0))

    out_ref[tiles, pl.ds(first + rows, HALO), :] = rim(from_corners[0], from_corners[1])
    out_ref[tiles, pl.ds(SUB, HALO), :] = rim(from_corners[2], from_corners[3])
    for pack in range(rows // LANES):
        right = from_cols[0, pl.ds(pack * HALO, HALO), :]
        left = from_cols[1, pl.ds(pack * HALO, HALO), :]
        for b in range(group):
            turn_right = (LANES - b * HALO) % LANES
            turn_left = (LANES - HALO - b * HALO) % LANES
            out_ref[tiles, pl.ds(first + pack * LANES + b * HALO, HALO), :] = rim(
                pltpu.roll(right, turn_right, 1) if turn_right else right,
                pltpu.roll(left, turn_left, 1) if turn_left else left,
            )

    for k in order:

        @pl.when(exists(*DIRECTIONS[k]))
        def _():
            copy(k).wait_send()


def cycles_kernel(
    peers, obst_hbm, load_hbm, rows_hbm, cols_hbm, out_ref,
    obst_ref, load_ref, exit_rows_ref, exit_cols_ref, source_ref,
    open_ref, marks_ref, diag_ref, first_ref, second_ref, rest_ref, shift_ref,
    expand_ref, corr_ref, fixed_ref, last_ref,
    top, bot, lef, rig, from_rows, from_cols, from_corners, input_sem, send_sem, recv_sem,
):
    goals, rows, cols = out_ref.shape
    tiles = cols // LANES
    span = tiles + 1
    ring = span * LANES
    wide = rows + 2 * HALO
    groups = wide // SUB
    coarse_rows = wide // COARSEN
    row_start = lax.axis_index("gx") * rows
    col_start = lax.axis_index("gy") * cols
    lane = lane_iota(SUB)
    sub = lax.broadcasted_iota(jnp.int32, (SUB, LANES), 0)
    coefficients = smoother_coefficients()
    inverse = 1.0 / CENTER

    def beside(center):
        up = [pltpu.roll(c, 1, 1) for c in center]
        down = [pltpu.roll(c, LANES - 1, 1) for c in center]
        return [
            jnp.where(lane == 0, up[t - 1], up[t])
            + jnp.where(lane == LANES - 1, down[(t + 1) % len(center)], down[t])
            for t in range(len(center))
        ]

    def load(ref, at, *lead):
        return [ref[(*lead, t, pl.ds(at, SUB), slice(None))] for t in range(span)]

    def cross(ref, at, *lead):
        center = load(ref, at, *lead)
        below = load(ref, at + 1, *lead)
        above = load(ref, at - 1, *lead)
        side = beside(center)
        return center, [below[t] + above[t] + side[t] for t in range(span)]

    def loop(low, high):
        def run(body):
            def step(i, carry):
                body(i, pl.multiple_of(i * SUB + SUB, SUB))
                return carry

            count = high - low
            unroll = max(u for u in range(1, UNROLL + 1) if count % u == 0)
            lax.fori_loop(low, high, step, 0, unroll=unroll)

        return run

    def meanwhile():
        zero = jnp.zeros((SUB, LANES), jnp.float32)
        for ends in (0, wide + SUB):
            for t in range(span):
                open_ref[t, pl.ds(ends, SUB), :] = zero
                corr_ref[t, pl.ds(ends, SUB), :] = zero
                for g in range(goals):
                    for ref in (first_ref, second_ref):
                        ref[g, t, pl.ds(ends, SUB), :] = zero

        count = exit_rows_ref.shape[1]
        row_of = lax.broadcasted_iota(jnp.int32, (wide, count), 0) + (row_start - HALO)
        ring_lane = lax.broadcasted_iota(jnp.int32, (ring, count), 0)
        col_of = jnp.where(ring_lane < cols + LANES // 2, ring_lane, ring_lane - ring) + col_start
        for g in range(goals):
            row_hot = (row_of == exit_rows_ref[pl.ds(g, 1), :]).astype(jnp.float32)
            col_hot = (col_of == exit_cols_ref[pl.ds(g, 1), :]).astype(jnp.float32)
            marks = lax.dot_general(
                row_hot.astype(jnp.bfloat16), col_hot.astype(jnp.bfloat16),
                (((1,), (1,)), ((), ())), preferred_element_type=jnp.float32,
            )
            for t in range(span):
                marks_ref[g, t] = marks[:, t * LANES : (t + 1) * LANES]

    pairs = (
        (obst_hbm, obst_ref), (load_hbm, load_ref), (rows_hbm, exit_rows_ref),
        (cols_hbm, exit_cols_ref),
    )
    inputs = [
        pltpu.make_async_copy(there, here, input_sem.at[k]) for k, (there, here) in enumerate(pairs)
    ]
    exchange(
        peers, inputs, obst_ref, load_ref, source_ref, top, bot, lef, rig, from_rows, from_cols,
        from_corners, send_sem, recv_sem, meanwhile,
    )

    @loop(0, groups)
    def _(i, at):
        for t in range(span):
            open_ref[t, pl.ds(at, SUB), :] = (source_ref[t, pl.ds(at, SUB), :] > 0.0).astype(
                jnp.float32
            )

    fine = lax.broadcasted_iota(jnp.int32, (ring, LANES), 0)
    fine = jnp.where(fine < cols + LANES // 2, fine, fine - ring + COARSEN * LANES) // COARSEN
    belongs = (fine == lax.broadcasted_iota(jnp.int32, (ring, LANES), 1)).astype(jnp.float32)

    belongs = belongs.astype(jnp.bfloat16)

    def split(value):
        high = value.astype(jnp.bfloat16)
        low = (value - high.astype(jnp.float32)).astype(jnp.bfloat16)
        return jnp.concatenate([high, low], axis=0)

    def product(value, matrix, dims):
        both = lax.dot_general(
            split(value), matrix, (dims, ((), ())), preferred_element_type=jnp.float32
        )
        size = value.shape[0]
        return both[:size] + both[size:]

    def restrict(ref, offset, leads):
        stacked = []
        for t in range(span):
            blocks = []
            for lead in leads:
                part = [
                    ref[(*lead, t, pl.ds(offset + k, coarse_rows, stride=COARSEN), slice(None))]
                    for k in range(COARSEN)
                ]
                blocks.append((part[0] + part[1]) + (part[2] + part[3]))
            stacked.append(jnp.concatenate(blocks, axis=0) if len(blocks) > 1 else blocks[0])
        total = product(jnp.concatenate(stacked, axis=1), belongs, ((1,), (0,)))
        return total * (1.0 / (COARSEN * COARSEN))

    shape = (coarse_rows, LANES)
    coarse_row = lax.broadcasted_iota(jnp.int32, shape, 0) - COARSE_HALO + row_start // COARSEN
    coarse_lane = lax.broadcasted_iota(jnp.int32, shape, 1)
    coarse_col = (
        jnp.where(coarse_lane < cols // COARSEN + LANES // 8, coarse_lane, coarse_lane - LANES)
        + col_start // COARSEN
    )
    floor = (
        (coarse_row >= 0) & (coarse_row < peers[0] * rows // COARSEN)
        & (coarse_col >= 0) & (coarse_col < peers[1] * cols // COARSEN)
    ).astype(jnp.float32)

    def coarse_solve(rhs):
        center_weight = 4.0 + COARSE_SHIFT
        gain = DAMPING / center_weight
        size = rhs.shape[0]
        inside = jnp.concatenate([floor] * (size // coarse_rows), axis=0)
        estimate = gain * rhs * inside
        for sweep in range(CSWEEPS - 1):
            around = (
                pltpu.roll(estimate, size - 1, 0) + pltpu.roll(estimate, 1, 0)
                + pltpu.roll(estimate, LANES - 1, 1) + pltpu.roll(estimate, 1, 1)
            )
            estimate = ((1.0 - DAMPING) * estimate + gain * (rhs + around)) * inside
        return estimate

    def spread(ref, i, t, *lead):
        even = jnp.broadcast_to(ref[(*lead, t, pl.ds(2 * i, 1), slice(None))], (SUB, LANES))
        odd = jnp.broadcast_to(ref[(*lead, t, pl.ds(2 * i + 1, 1), slice(None))], (SUB, LANES))
        return jnp.where(sub < COARSEN, even, odd)

    fine_columns = product(coarse_solve(restrict(source_ref, SUB, [()])), belongs, ((1,), (1,)))
    for t in range(span):
        expand_ref[t] = fine_columns[:, t * LANES : (t + 1) * LANES]

    @loop(0, groups)
    def _(i, at):
        opened, around = cross(open_ref, at)
        source, source_around = cross(source_ref, at)
        for t in range(span):
            base = SCREENING + 4.0 * (1.0 - opened[t]) + opened[t] * around[t]
            mixed = (coefficients[3] * inverse) * opened[t] * source_around[t]
            mixed = mixed + coefficients[2] * source[t]
            lifted = coefficients[3] * source[t]
            sink = EXIT_SINK * opened[t]
            corr_ref[t, pl.ds(at, SUB), :] = opened[t] * spread(expand_ref, i, t)
            for g in range(goals):
                exits = jnp.minimum(marks_ref[g, t, pl.ds(i * SUB, SUB), :], 1.0)
                kept = 1.0 - (base + sink * exits) * inverse
                diag_ref[g, t, pl.ds(at, SUB), :] = kept
                first_ref[g, t, pl.ds(at, SUB), :] = kept * lifted + mixed

    def horner(old_ref, new_ref, coefficient, rhs):
        def body(i, at):
            weight = [inverse * open_ref[t, pl.ds(at, SUB), :] for t in range(span)]
            for g in range(goals):
                center, around = cross(old_ref, at, g)
                for t in range(span):
                    kept = diag_ref[g, t, pl.ds(at, SUB), :]
                    new_ref[g, t, pl.ds(at, SUB), :] = (
                        kept * center[t] + weight[t] * around[t] + coefficient * rhs(g, t, at)
                    )

        return body

    plain = lambda g, t, at: source_ref[t, pl.ds(at, SUB), :]
    loop(0, groups)(horner(first_ref, second_ref, coefficients[1], plain))
    loop(0, groups)(horner(second_ref, first_ref, coefficients[0], plain))

    @loop(0, groups)
    def _(i, at):
        correction, around_corr = cross(corr_ref, at)
        opened = load(open_ref, at)
        for g in range(goals):
            center, around = cross(first_ref, at, g)
            for t in range(span):
                kept = CENTER * (diag_ref[g, t, pl.ds(at, SUB), :] - 1.0)
                residual = (
                    source_ref[t, pl.ds(at, SUB), :] + kept * center[t] + opened[t] * around[t]
                )
                rest_ref[g, t, pl.ds(i * SUB, SUB), :] = residual
                shift_ref[g, t, pl.ds(at, SUB), :] = (
                    residual + kept * correction[t] + opened[t] * around_corr[t]
                )

    estimates = coarse_solve(restrict(rest_ref, 0, [(g,) for g in range(goals)]))
    fine_columns = product(estimates, belongs[:cols], ((1,), (1,)))
    for g in range(goals):
        for t in range(tiles):
            last_ref[g, t] = fine_columns[
                g * coarse_rows : (g + 1) * coarse_rows, t * LANES : (t + 1) * LANES
            ]

    edge = HALO // SUB

    @loop(edge - 1, groups - edge + 1)
    def _(i, at):
        weight = [(coefficients[3] * inverse) * open_ref[t, pl.ds(at, SUB), :] for t in range(span)]
        for g in range(goals):
            center, around = cross(shift_ref, at, g)
            for t in range(span):
                kept = diag_ref[g, t, pl.ds(at, SUB), :]
                second_ref[g, t, pl.ds(at, SUB), :] = (
                    (coefficients[3] * kept + coefficients[2]) * center[t] + weight[t] * around[t]
                )

    shifted = lambda g, t, at: shift_ref[g, t, pl.ds(at, SUB), :]
    loop(edge - 1, groups - edge + 1)(horner(second_ref, fixed_ref, coefficients[1], shifted))

    @loop(edge, groups - edge)
    def _(i, at):
        opened = load(open_ref, at)
        for g in range(goals):
            center, around = cross(fixed_ref, at, g)
            for t in range(tiles):
                kept = diag_ref[g, t, pl.ds(at, SUB), :]
                smooth = (
                    kept * center[t] + (inverse * opened[t]) * around[t]
                    + coefficients[0] * shift_ref[g, t, pl.ds(at, SUB), :]
                )
                out_ref[g, pl.ds(pl.multiple_of(at - SUB - HALO, SUB), SUB), pl.ds(t * LANES, LANES)] = (
                    first_ref[g, t, pl.ds(at, SUB), :] + corr_ref[t, pl.ds(at, SUB), :]
                    + smooth + opened[t] * spread(last_ref, i, t, g)
                )


def per_device(peers, obstacles, load, exit_rows, exit_cols):
    rows, cols = obstacles.shape
    goals = exit_rows.shape[0]
    tiles = cols // LANES
    span = tiles + 1
    wide = rows + 2 * HALO
    padded = wide + 2 * SUB
    f32 = jnp.float32
    vmem = pl.BlockSpec(memory_space=pltpu.VMEM)
    packed = rows * HALO // LANES
    exits = exit_rows.shape
    field = pltpu.VMEM((goals, span, padded, LANES), f32)
    flat = pltpu.VMEM((goals, span, wide, LANES), f32)
    shared = pltpu.VMEM((span, padded, LANES), f32)
    coarse = wide // COARSEN
    return pl.pallas_call(
        functools.partial(cycles_kernel, peers),
        out_shape=jax.ShapeDtypeStruct((goals, rows, cols), f32),
        in_specs=[pl.BlockSpec(memory_space=pltpu.HBM)] * 4,
        out_specs=vmem,
        scratch_shapes=[
            pltpu.VMEM((rows, cols), jnp.int32),
            pltpu.VMEM((rows, cols), f32),
            pltpu.VMEM(exits, jnp.int32),
            pltpu.VMEM(exits, jnp.int32),
            shared,
            shared, flat, field, field, field, flat, field,
            pltpu.VMEM((span, coarse, LANES), f32), shared, field,
            pltpu.VMEM((goals, tiles, coarse, LANES), f32),
            pltpu.VMEM((tiles, HALO, LANES), f32),
            pltpu.VMEM((tiles, HALO, LANES), f32),
            pltpu.VMEM((packed, LANES), f32),
            pltpu.VMEM((packed, LANES), f32),
            pltpu.VMEM((2, tiles, HALO, LANES), f32),
            pltpu.VMEM((2, packed, LANES), f32),
            pltpu.VMEM((4, HALO, LANES), f32),
            pltpu.SemaphoreType.DMA((4,)),
            pltpu.SemaphoreType.DMA((len(DIRECTIONS),)),
            pltpu.SemaphoreType.DMA((len(DIRECTIONS),)),
        ],
        compiler_params=pltpu.CompilerParams(
            collective_id=0, has_side_effects=True, vmem_limit_bytes=48 * 1024 * 1024
        ),
        name="cycles",
    )(*(pltpu.with_memory_space_constraint(x, pltpu.HBM) for x in (obstacles, load, exit_rows, exit_cols)))


def solution(mesh):
    peers = (mesh.shape["gx"], mesh.shape["gy"])
    return jax.shard_map(
        functools.partial(per_device, peers),
        mesh=mesh,
        in_specs=(P("gx", "gy"), P("gx", "gy"), P(), P()),
        out_specs=P(None, "gx", "gy"),
        check_vma=False,
    )
```
